32 devices in a mesh: pool: 4 (over x, core), rp: 8 (over z, y).
Axes of the slice: x: 2, y: 2, z: 4, core: 2. Of those that a mesh axis runs over, the one named last changes fastest.
Arguments:
- wannier_coupling: bfloat16 [2, 512, 5184], P(None, ('pool', 'rp')), may hold values from -0.25 to 0.25
- lattice_vectors: int32 [3, 512], P(None, ('pool', 'rp')), may hold values from -12 to 12
- degeneracy: int32 [1, 512], P(None, ('pool', 'rp')), may hold values from 1 to 4
- fine_points: int32 [3, 32], P(None, 'pool'), may hold values from 0 to 47
- mode_vectors: float32 [32, 2, 9, 9], P('pool'), may hold values from -2 to 2
- bands_shifted: float32 [32, 2, 24, 24], P(('pool', 'rp')), may hold values from -1.25 to 1.25
- bands_anchor: float32 [2, 24, 24], replicated, may hold values from -1.25 to 1.25
Outputs:
- coupling: float32 [32, 2, 9, 576], P(('pool', 'rp'))
The draws below stay inside these ranges and needn't reach their ends.
All inputs are finite; a program needn't handle non-finite values.
Results may differ from the reference program's by a relative error of at most 0.0021.
Values may be sent and summed in bfloat16 or wider, within the bound.
A program may use at most 64 MiB of HBM per device.

```python
import math
import jax
import jax.numpy as jnp
from jax import lax

NB = 24
MODES = 9
NQG = 48
RMAX = 12
RP_DEV = 16
QPTS = 32
RPTS = 512
COLS = 5184
DEVICES = 32


def plant(result, key, least, high):
    extent = result.shape
    index_at = [jax.random.randint(jax.random.fold_in(key, axis), (), 0, extent[axis]) for axis in range(len(extent))]
    result = result.at[tuple(index_at)].set(least)
    longest = extent.index(max(extent))
    index_at[longest] = (index_at[longest] + 1) % extent[longest]
    return result.at[tuple(index_at)].set(high)


def block_levels(stream_key, dims, pieces, smallest, top_value):
    gain, own = 1.0, jax.random.fold_in(stream_key, 6)
    for dim, parts in pieces:
        heights = jnp.exp(jax.random.uniform(jax.random.fold_in(own, dim), (parts,), jnp.float32, smallest / len(pieces), top_value / len(pieces)))
        gain = gain * jnp.repeat(heights, dims[dim] // parts).reshape([-1 if axis == dim else 1 for axis in range(len(dims))])
    return gain


def gaussian(own_key, extent, deviation, limit, cuts=(), kind=jnp.bfloat16):
    result = jax.random.normal(own_key, extent, jnp.float32) * deviation
    if len(cuts) > 0:
        result = block_levels(own_key, extent, cuts, -0.22, 0.18) * result
    return jnp.clip(result, min=-limit, max=limit).astype(kind)


def setup_inputs(seed: int = 0) -> dict:
    arg_keys = jax.random.split(jax.random.key(seed), 8)
    wannier_coupling = gaussian(arg_keys[0], (2, RPTS, COLS), RPTS ** -0.5, 0.25, ((1, 32),))
    lattice_vectors = plant(jax.random.randint(arg_keys[1], (3, RPTS), 0 - RMAX, RMAX + 1), jax.random.fold_in(arg_keys[1], 1), 0 - RMAX, RMAX).astype(jnp.int32)
    degeneracy = plant(jax.random.randint(arg_keys[2], (1, RPTS), 1, 5), jax.random.fold_in(arg_keys[2], 1), 1, 4).astype(jnp.int32)
    fine_points = plant(jax.random.randint(arg_keys[3], (3, QPTS), 0, NQG), jax.random.fold_in(arg_keys[3], 1), 0, NQG - 1).astype(jnp.int32)
    mode_vectors = gaussian(arg_keys[4], (QPTS, 2, MODES, MODES), 0.33, 2.0, ((0, 4),), jnp.float32)
    bands_shifted = gaussian(arg_keys[5], (QPTS, 2, NB, NB), NB ** -0.5, 1.25, ((0, 32),), jnp.float32)
    bands_anchor = gaussian(arg_keys[6], (2, NB, NB), NB ** -0.5, 1.25, (), jnp.float32)
    return dict(wannier_coupling=wannier_coupling, lattice_vectors=lattice_vectors, degeneracy=degeneracy, fine_points=fine_points, mode_vectors=mode_vectors, bands_shifted=bands_shifted, bands_anchor=bands_anchor)


full_turn = 2.0 * math.pi
highest = lax.Precision.HIGHEST


def phase_pair(fine_points, lattice_vectors, degeneracy):
    winding = fine_points[0][:, None] * lattice_vectors[0][None, :]
    winding = winding + fine_points[1][:, None] * lattice_vectors[1][None, :]
    winding = winding + fine_points[2][:, None] * lattice_vectors[2][None, :]
    winding = jnp.mod(winding, NQG)
    angles = winding.astype(jnp.float32) * (full_turn / NQG)
    weights = 1.0 / degeneracy[0].astype(jnp.float32)
    phase_real = (jnp.cos(angles) * weights[None, :]).astype(jnp.bfloat16)
    phase_imag = (jnp.sin(angles) * weights[None, :]).astype(jnp.bfloat16)
    return phase_real, phase_imag


def contract_modes(source, matrix):
    return jnp.einsum("qap,qav->qvp", source, matrix, precision=highest)


def rotate_modes(real_part, imag_part, vectors):
    vector_real = vectors[:, 0]
    vector_imag = vectors[:, 1]
    out_real = contract_modes(real_part, vector_real) - contract_modes(imag_part, vector_imag)
    out_imag = contract_modes(real_part, vector_imag) + contract_modes(imag_part, vector_real)
    return out_real, out_imag


def rotate_bands(real_part, imag_part, shifted, anchor):
    points = real_part.shape[0]
    mode_count = real_part.shape[1]
    band_count = anchor.shape[1]
    grid_real = real_part.reshape(points, mode_count, band_count, band_count)
    grid_imag = imag_part.reshape(points, mode_count, band_count, band_count)

    def right_product(source, matrix):
        return jnp.einsum("qvmn,nl->qvml", source, matrix, precision=highest)

    def left_product(matrix, source):
        return jnp.einsum("qma,qvml->qval", matrix, source, precision=highest)

    right_real = right_product(grid_real, anchor[0]) - right_product(grid_imag, anchor[1])
    right_imag = right_product(grid_real, anchor[1]) + right_product(grid_imag, anchor[0])
    shift_real = shifted[:, 0]
    shift_imag = shifted[:, 1]
    final_real = left_product(shift_real, right_real) + left_product(shift_imag, right_imag)
    final_imag = left_product(shift_real, right_imag) - left_product(shift_imag, right_real)
    final_real = final_real.reshape(points, mode_count, band_count * band_count)
    final_imag = final_imag.reshape(points, mode_count, band_count * band_count)
    return jnp.stack([final_real, final_imag], axis=1)


def reference(wannier_coupling, lattice_vectors, degeneracy, fine_points, mode_vectors, bands_shifted, bands_anchor):
    phase_real, phase_imag = phase_pair(fine_points, lattice_vectors, degeneracy)
    block = RP_DEV * 8
    columns = wannier_coupling.shape[2]
    points = fine_points.shape[1]

    def accumulate(totals, index):
        begin = (index * block).astype(jnp.int32)
        coupling_rows = lax.dynamic_slice_in_dim(wannier_coupling, begin, block, 1).astype(jnp.float32)
        left_real = lax.dynamic_slice_in_dim(phase_real, begin, block, 1).astype(jnp.float32)
        left_imag = lax.dynamic_slice_in_dim(phase_imag, begin, block, 1).astype(jnp.float32)
        real_sum = totals[0] + jnp.dot(left_real, coupling_rows[0], precision=highest) - jnp.dot(left_imag, coupling_rows[1], precision=highest)
        imag_sum = totals[1] + jnp.dot(left_real, coupling_rows[1], precision=highest) + jnp.dot(left_imag, coupling_rows[0], precision=highest)
        return (real_sum, imag_sum), None

    initial = jnp.zeros((points, columns), jnp.float32)
    sums, unused = lax.scan(accumulate, (initial, initial), jnp.arange(DEVICES // 8, dtype=jnp.int32))
    mode_count = mode_vectors.shape[2]
    sum_real = sums[0].reshape(points, mode_count, -1)
    sum_imag = sums[1].reshape(points, mode_count, -1)
    mode_real, mode_imag = rotate_modes(sum_real, sum_imag, mode_vectors)
    return rotate_bands(mode_real, mode_imag, bands_shifted, bands_anchor)
```

```python
import functools
import math

import jax
import jax.numpy as jnp
from jax import lax
from jax.experimental import pallas as pl
from jax.experimental.pallas import tpu as pltpu
from jax.sharding import PartitionSpec as P

NQG = 48
LANES = 128
SPAN = 1024
WIRE = jnp.float32

full_turn = 2.0 * math.pi
highest = lax.Precision.HIGHEST
MESH = pl.DeviceIdType.MESH


def split_wide(value):
    high = value.astype(jnp.bfloat16)
    low = (value - high.astype(jnp.float32)).astype(jnp.bfloat16)
    return high, low


def build_pairs(shifted_ref, anchor_ref, kron):
    bands = anchor_ref.shape[1]
    pairs = bands * bands
    row = lax.broadcasted_iota(jnp.int32, (bands, pairs), 0).astype(jnp.float32)
    col = lax.broadcasted_iota(jnp.int32, (bands, pairs), 1).astype(jnp.float32)
    outer = jnp.floor((col + 0.5) * (1.0 / bands))
    inner = col - outer * bands
    pick_outer = jnp.where(row == outer, 1.0, 0.0)
    pick_inner = jnp.where(row == inner, 1.0, 0.0)

    def spread(matrix, pick):
        return jnp.dot(matrix, pick, precision=highest, preferred_element_type=jnp.float32)

    shift_real = spread(shifted_ref[0, 0], pick_outer)
    shift_imag = spread(shifted_ref[0, 1], pick_outer)
    anchor_real = spread(anchor_ref[0], pick_inner)
    anchor_imag = spread(anchor_ref[1], pick_inner)
    for start in range(0, bands, 2):
        reals, imags = [], []
        for m in (start, start + 1):
            sr = shift_real[m : m + 1]
            si = shift_imag[m : m + 1]
            reals.append(sr * anchor_real + si * anchor_imag)
            imags.append(sr * anchor_imag - si * anchor_real)
        rows = pl.ds(start * bands, 2 * bands)
        kron[0, rows, :], kron[1, rows, :] = split_wide(jnp.concatenate(reals, axis=0))
        kron[2, rows, :], kron[3, rows, :] = split_wide(jnp.concatenate(imags, axis=0))


def kernel(
    pool,
    rp,
    coupling_ref,
    lattice_ref,
    points_ref,
    modes_ref,
    shifted_ref,
    anchor_ref,
    out_ref,
    rows_all,
    lattice_pair,
    points_all,
    partial,
    wire,
    recv,
    flat,
    kron,
    local_sem,
    pair_send,
    pair_recv,
    small_send,
    small_recv,
    point_send,
    point_recv,
    send_sem,
    recv_sem,
):
    sides = pool // 2
    my_pool = lax.axis_index("pool")
    my_rp = lax.axis_index("rp")
    core = lax.rem(my_pool, 2)
    side = my_pool // 2
    partner = side * 2 + 1 - core
    total = sides * rp
    me = side * rp + my_rp
    points = points_ref.shape[0]

    barrier = pltpu.get_barrier_semaphore()
    pl.semaphore_signal(barrier, inc=1, device_id={"pool": partner, "rp": my_rp}, device_id_type=MESH)

    def target(step):
        other = lax.rem(me + step, total)
        return other, {"pool": (other // rp) * 2 + core, "rp": lax.rem(other, rp)}

    for step in range(1, total):
        pl.semaphore_signal(barrier, inc=1, device_id=target(step)[1], device_id_type=MESH)

    load = pltpu.make_async_copy(coupling_ref, rows_all.at[0], local_sem)
    load.start()
    here = pl.ds(pl.multiple_of(side * points, points), points)
    points_all[here, :] = points_ref[...]

    pl.semaphore_wait(barrier, total)

    pair_id = {"pool": partner, "rp": my_rp}
    small_copy = pltpu.make_async_remote_copy(
        src_ref=lattice_ref, dst_ref=lattice_pair, send_sem=small_send, recv_sem=small_recv,
        device_id=pair_id, device_id_type=MESH)
    small_copy.start()
    point_copies = []
    for step in range(1, sides):
        other_side = lax.rem(side + step, sides)
        copy = pltpu.make_async_remote_copy(
            src_ref=points_ref, dst_ref=points_all.at[here, :],
            send_sem=point_send.at[step - 1], recv_sem=point_recv.at[step - 1],
            device_id={"pool": other_side * 2 + core, "rp": my_rp}, device_id_type=MESH)
        copy.start()
        point_copies.append(copy)
    pair_copy = pltpu.make_async_remote_copy(
        src_ref=coupling_ref, dst_ref=rows_all.at[1], send_sem=pair_send, recv_sem=pair_recv,
        device_id=pair_id, device_id_type=MESH)
    pair_copy.start()

    build_pairs(shifted_ref, anchor_ref, kron)

    small_copy.wait()
    for copy in point_copies:
        copy.wait()
    here_rows = coupling_ref.shape[1]
    fine = points_all[...]

    def phases(lattice):
        winding = fine[:, 0:1] * lattice[0:1, :] + fine[:, 1:2] * lattice[1:2, :] + fine[:, 2:3] * lattice[2:3, :]
        winding = winding - NQG * jnp.floor((winding + 0.5) * (1.0 / NQG))
        angles = winding * (full_turn / NQG)
        weights = 1.0 / lattice[3:4, :]
        return (jnp.cos(angles) * weights)[:, :here_rows], (jnp.sin(angles) * weights)[:, :here_rows]

    own_real, own_imag = phases(lattice_ref[...])
    far_real, far_imag = phases(lattice_pair[...])
    left_real = jnp.concatenate([own_real, -own_imag, far_real, -far_imag], axis=1)
    left_imag = jnp.concatenate([own_imag, own_real, far_imag, far_real], axis=1)
    left = jnp.concatenate([left_real, left_imag], axis=0).astype(jnp.bfloat16)
    half = left_real.shape[0]

    load.wait()
    pair_copy.wait()
    columns = coupling_ref.shape[2]
    height = recv.shape[1]
    for first in range(0, columns, SPAN):
        count = min(SPAN, columns - first)
        block = rows_all[:, :, :, first : first + count].reshape(4 * here_rows, count)
        product = jnp.dot(left, block, preferred_element_type=jnp.float32)
        for begin in range(0, count, LANES):
            size = min(LANES, count - begin)
            piece = product[:, begin : begin + size]
            if size < LANES:
                piece = jnp.concatenate([piece, jnp.zeros((2 * half, LANES - size), jnp.float32)], axis=1)
            row = (first + begin) // LANES * 2
            for part in range(2):
                partial[pl.ds(row + part, half, stride=height), :] = piece[part * half : (part + 1) * half]

    source = partial
    if WIRE != jnp.float32:
        wire[...] = partial[...].astype(WIRE)
        source = wire

    copies = []
    for step in range(1, total):
        other, other_id = target(step)
        rows = pl.ds(pl.multiple_of(other * height, height), height)
        copy = pltpu.make_async_remote_copy(
            src_ref=source.at[rows, :], dst_ref=recv.at[step],
            send_sem=send_sem.at[step], recv_sem=recv_sem.at[step],
            device_id=other_id, device_id_type=MESH)
        copy.start()
        copies.append(copy)

    folded = partial[pl.ds(pl.multiple_of(me * height, height), height), :]
    for step in range(1, total):
        copies[step - 1].wait_recv()
        folded = folded + recv[step].astype(jnp.float32)
    for tile in range(flat.shape[1] // LANES):
        flat[:, tile * LANES : (tile + 1) * LANES] = folded[2 * tile : 2 * tile + 2]

    mode_count = modes_ref.shape[3]
    pairs = out_ref.shape[3]
    window = -(-(pairs + LANES // 2) // LANES) * LANES
    vectors_real = modes_ref[my_rp, 0]
    vectors_imag = modes_ref[my_rp, 1]
    moded_real = jnp.zeros((vectors_real.shape[0], pairs), jnp.float32)
    moded_imag = moded_real
    for a in range(mode_count):
        offset = a * pairs % LANES
        begin = a * pairs - offset
        value = flat[:, begin : begin + window]
        if offset:
            value = pltpu.roll(value, window - offset, 1)
        value = value[:, :pairs]
        fr, fi = value[0:1], value[1:2]
        vr, vi = vectors_real[:, a : a + 1], vectors_imag[:, a : a + 1]
        moded_real = moded_real + vr * fr - vi * fi
        moded_imag = moded_imag + vi * fr + vr * fi
    pad = moded_real.shape[0]
    high, low = split_wide(jnp.concatenate([moded_real, moded_imag], axis=0))
    both = jnp.concatenate([high, low], axis=0)

    def product(index):
        first = jnp.dot(both, kron[index], preferred_element_type=jnp.float32)
        second = jnp.dot(high, kron[index + 1], preferred_element_type=jnp.float32)
        return first[: 2 * pad] + first[2 * pad :] + second

    by_real = product(0)
    by_imag = product(2)
    out_ref[0, 0] = (by_real[:pad] - by_imag[pad:])[:mode_count]
    out_ref[0, 1] = (by_imag[:pad] + by_real[pad:])[:mode_count]
    for copy in copies:
        copy.wait_send()


def per_device(
    pool,
    rp,
    wannier_coupling,
    lattice_vectors,
    degeneracy,
    fine_points,
    mode_vectors,
    bands_shifted,
    bands_anchor,
):
    rows_here, columns = wannier_coupling.shape[1:]
    points = fine_points.shape[1]
    mode_count = mode_vectors.shape[2]
    pairs = columns // mode_count
    lattice = jnp.concatenate([lattice_vectors, degeneracy], axis=0).astype(jnp.float32)
    lattice = jnp.pad(lattice, ((0, 4), (0, LANES - rows_here)), constant_values=1.0)
    fine = jnp.pad(fine_points.astype(jnp.float32).T, ((0, 0), (0, LANES - 3)))
    pad_modes = -(-mode_count // 8) * 8
    modes = jnp.pad(jnp.swapaxes(mode_vectors, 2, 3), ((0, 0), (0, 0), (0, pad_modes - mode_count), (0, 0)))
    sides = pool // 2
    total = sides * rp
    tiles = -(-columns // LANES)
    height = -(-2 * tiles // 8) * 8
    vmem = pl.BlockSpec(memory_space=pltpu.VMEM)
    dma = pltpu.SemaphoreType.DMA
    return pl.pallas_call(
        functools.partial(kernel, pool, rp),
        out_shape=jax.ShapeDtypeStruct((1, 2, mode_count, pairs), jnp.float32),
        in_specs=[pl.BlockSpec(memory_space=pl.ANY)] + [vmem] * 5,
        out_specs=vmem,
        scratch_shapes=[
            pltpu.VMEM((2, 2, rows_here, columns), jnp.bfloat16),
            pltpu.VMEM(lattice.shape, jnp.float32),
            pltpu.VMEM((sides * points, LANES), jnp.float32),
            pltpu.VMEM((total * height, LANES), jnp.float32),
            pltpu.VMEM((total * height, LANES), WIRE) if WIRE != jnp.float32 else pltpu.VMEM((16, LANES), WIRE),
            pltpu.VMEM((total, height, LANES), WIRE),
            pltpu.VMEM((2, tiles * LANES), jnp.float32),
            pltpu.VMEM((4, pairs, pairs), jnp.bfloat16),
            dma, dma, dma, dma, dma,
            dma((sides - 1,)), dma((sides - 1,)),
            dma((total,)), dma((total,)),
        ],
        compiler_params=pltpu.CompilerParams(
            collective_id=0, has_side_effects=True, vmem_limit_bytes=48 * 1024 * 1024
        ),
    )(wannier_coupling, lattice, fine, modes, bands_shifted, bands_anchor)


def solution(mesh):
    return jax.shard_map(
        functools.partial(per_device, mesh.shape["pool"], mesh.shape["rp"]),
        mesh=mesh,
        in_specs=(
            P(None, ("pool", "rp"), None),
            P(None, ("pool", "rp")),
            P(None, ("pool", "rp")),
            P(None, "pool"),
            P("pool", None, None, None),
            P(("pool", "rp"), None, None, None),
            P(),
        ),
        out_specs=P(("pool", "rp"), None, None, None),
        check_vma=False,
    )
```

```python
import functools
import math

import jax
import jax.numpy as jnp
from jax import lax
from jax.experimental import pallas as pl
from jax.experimental.pallas import tpu as pltpu
from jax.sharding import PartitionSpec as P

NQG = 48
LANES = 128
SPAN = 1024
WIRE = jnp.int16
TOP = 32000.0

full_turn = 2.0 * math.pi
highest = lax.Precision.HIGHEST
MESH = pl.DeviceIdType.MESH


def split_wide(value):
    high = value.astype(jnp.bfloat16)
    low = (value - high.astype(jnp.float32)).astype(jnp.bfloat16)
    return high, low


def build_pairs(shifted_ref, anchor_ref, kron):
    bands = anchor_ref.shape[1]
    pairs = bands * bands
    row = lax.broadcasted_iota(jnp.int32, (bands, pairs), 0).astype(jnp.float32)
    col = lax.broadcasted_iota(jnp.int32, (bands, pairs), 1).astype(jnp.float32)
    outer = jnp.floor((col + 0.5) * (1.0 / bands))
    inner = col - outer * bands
    pick_outer = jnp.where(row == outer, 1.0, 0.0)
    pick_inner = jnp.where(row == inner, 1.0, 0.0)

    def spread(matrix, pick):
        return jnp.dot(matrix, pick, precision=highest, preferred_element_type=jnp.float32)

    shift_real = spread(shifted_ref[0, 0], pick_outer)
    shift_imag = spread(shifted_ref[0, 1], pick_outer)
    anchor_real = spread(anchor_ref[0], pick_inner)
    anchor_imag = spread(anchor_ref[1], pick_inner)
    for start in range(0, bands, 2):
        reals, imags = [], []
        for m in (start, start + 1):
            sr = shift_real[m : m + 1]
            si = shift_imag[m : m + 1]
            reals.append(sr * anchor_real + si * anchor_imag)
            imags.append(sr * anchor_imag - si * anchor_real)
        rows = pl.ds(start * bands, 2 * bands)
        kron[0, rows, :], kron[1, rows, :] = split_wide(jnp.concatenate(reals, axis=0))
        kron[2, rows, :], kron[3, rows, :] = split_wide(jnp.concatenate(imags, axis=0))


def far_first(sides, rp):
    shifts = sorted(range(rp), key=lambda shift: -min(shift, rp - shift))
    return [(side, shift) for shift in shifts for side in reversed(range(sides)) if side or shift]


def kernel(
    pool,
    rp,
    coupling_ref,
    lattice_ref,
    weight_ref,
    points_ref,
    modes_ref,
    shifted_ref,
    anchor_ref,
    out_ref,
    rows_all,
    lattice,
    weight,
    points,
    modes,
    shifted,
    anchor,
    partial,
    wire,
    recv,
    flat,
    kron,
    load_sem,
    pair_send,
    pair_recv,
    point_send,
    point_recv,
    send_sem,
    recv_sem,
):
    sides = pool // 2
    my_pool = lax.axis_index("pool")
    my_rp = lax.axis_index("rp")
    core = lax.rem(my_pool, 2)
    side = my_pool // 2
    partner = side * 2 + 1 - core
    total = sides * rp
    order = far_first(sides, rp)
    pair_id = {"pool": partner, "rp": my_rp}

    def target(step):
        other_side = lax.rem(side + step[0], sides)
        other_rp = lax.rem(my_rp + step[1], rp)
        return other_side * rp + other_rp, {"pool": other_side * 2 + core, "rp": other_rp}

    barrier = pltpu.get_barrier_semaphore()
    for step in order:
        pl.semaphore_signal(barrier, inc=1, device_id=target(step)[1], device_id_type=MESH)
    pl.semaphore_signal(barrier, inc=1, device_id=pair_id, device_id_type=MESH)

    loads = []
    for number, (source, place) in enumerate((
        (coupling_ref, rows_all.at[0]),
        (lattice_ref, lattice.at[0]),
        (weight_ref, weight.at[0]),
        (points_ref, points.at[side]),
        (modes_ref.at[my_rp], modes),
        (shifted_ref, shifted),
        (anchor_ref, anchor),
    )):
        load = pltpu.make_async_copy(source, place, load_sem.at[number])
        load.start()
        loads.append(load)
    loads[5].wait()
    loads[6].wait()
    build_pairs(shifted, anchor, kron)
    for load in loads[:5]:
        load.wait()

    pl.semaphore_wait(barrier, total)

    copies = []
    for number, place in enumerate((lattice, weight, rows_all)):
        copy = pltpu.make_async_remote_copy(
            src_ref=place.at[0], dst_ref=place.at[1], send_sem=pair_send.at[number], recv_sem=pair_recv.at[number],
            device_id=pair_id, device_id_type=MESH)
        copy.start()
        copies.append(copy)
    for step in range(1, sides):
        other_side = lax.rem(side + step, sides)
        copy = pltpu.make_async_remote_copy(
            src_ref=points.at[side], dst_ref=points.at[side],
            send_sem=point_send.at[step - 1], recv_sem=point_recv.at[step - 1],
            device_id={"pool": other_side * 2 + core, "rp": my_rp}, device_id_type=MESH)
        copy.start()
        copies.append(copy)
    for copy in copies[:2] + copies[3:]:
        copy.wait()
    here_rows = coupling_ref.shape[1]

    def turn(left, right):
        return lax.dot_general(left, right, (((0,), (0,)), ((), ())), precision=highest, preferred_element_type=jnp.float32)

    def phases(which):
        vectors = lattice[which].astype(jnp.float32)
        winding = jnp.concatenate([turn(points[s].astype(jnp.float32), vectors) for s in range(sides)], axis=0)
        winding = jnp.floor(winding + 0.5)
        winding = winding - NQG * jnp.floor((winding + 0.5) * (1.0 / NQG))
        angles = winding * (full_turn / NQG)
        weights = 1.0 / weight[which].astype(jnp.float32)
        return jnp.cos(angles) * weights, jnp.sin(angles) * weights

    own_real, own_imag = phases(0)
    far_real, far_imag = phases(1)
    left_real = jnp.concatenate([own_real, -own_imag, far_real, -far_imag], axis=1)
    left_imag = jnp.concatenate([own_imag, own_real, far_imag, far_real], axis=1)
    left = jnp.concatenate([left_real, left_imag], axis=0).astype(jnp.bfloat16)
    half = left_real.shape[0]

    copies[2].wait()
    columns = coupling_ref.shape[2]
    height = recv.shape[1]
    largest = jnp.full((half, LANES), 1e-30, jnp.float32)
    for first in range(0, columns, SPAN):
        count = min(SPAN, columns - first)
        block = rows_all[:, :, :, first : first + count].reshape(4 * here_rows, count)
        product = jnp.dot(left, block, preferred_element_type=jnp.float32)
        for begin in range(0, count, LANES):
            size = min(LANES, count - begin)
            piece = product[:, begin : begin + size]
            if size < LANES:
                piece = jnp.concatenate([piece, jnp.zeros((2 * half, LANES - size), jnp.float32)], axis=1)
            row = (first + begin) // LANES * 2
            largest = jnp.maximum(largest, jnp.maximum(jnp.abs(piece[:half]), jnp.abs(piece[half:])))
            for part in range(2):
                partial[pl.ds(row + part, half, stride=height), :] = piece[part * half : (part + 1) * half]

    used = 2 * (-(-columns // LANES))
    largest = jnp.max(jnp.max(largest, axis=0, keepdims=True), axis=1, keepdims=True)
    exponent = jnp.ceil(jnp.log2(largest * (1.0 / TOP)) + 1e-3)
    inverse = jnp.broadcast_to(jnp.exp2(-exponent), (1, LANES))
    exponent = jnp.broadcast_to(exponent, (height, LANES))
    is_value = lax.broadcasted_iota(jnp.int32, (height, LANES), 0) < used

    copies = []
    for number, step in enumerate(order):
        other, other_id = target(step)
        rows = pl.ds(pl.multiple_of(other * height, 8), height)
        coded = jnp.where(is_value, partial[rows, :] * inverse, exponent)
        wire[number] = jnp.round(coded).astype(jnp.int32).astype(WIRE)
        copies.append(pltpu.make_async_remote_copy(
            src_ref=wire.at[number], dst_ref=recv.at[number],
            send_sem=send_sem.at[number], recv_sem=recv_sem.at[number],
            device_id=other_id, device_id_type=MESH))
        if number:
            copies[number - 1].start()
    copies[-1].start()

    me = side * rp + my_rp
    folded = partial[pl.ds(pl.multiple_of(me * height, 8), height), :]
    for number in reversed(range(len(order))):
        copies[number].wait_recv()
        coded = recv[number].astype(jnp.int32).astype(jnp.float32)
        folded = folded + coded * jnp.exp2(coded[used : used + 1])
    for tile in range(flat.shape[1] // LANES):
        flat[:, tile * LANES : (tile + 1) * LANES] = folded[2 * tile : 2 * tile + 2]

    mode_count = modes_ref.shape[3]
    pad = -(-mode_count // 8) * 8
    pairs = out_ref.shape[3]
    window = -(-(pairs + LANES // 2) // LANES) * LANES
    unit_row = lax.broadcasted_iota(jnp.int32, (mode_count, LANES), 0)
    unit_col = lax.broadcasted_iota(jnp.int32, (mode_count, LANES), 1)
    unit = jnp.where(unit_row == unit_col, 1.0, 0.0)
    empty = jnp.zeros((pad - mode_count, LANES), jnp.float32)
    vectors_real = jnp.concatenate([turn(modes[0], unit), empty], axis=0)
    vectors_imag = jnp.concatenate([turn(modes[1], unit), empty], axis=0)
    moded_real = jnp.zeros((vectors_real.shape[0], pairs), jnp.float32)
    moded_imag = moded_real
    for a in range(mode_count):
        offset = a * pairs % LANES
        begin = a * pairs - offset
        value = flat[:, begin : begin + window]
        if offset:
            value = pltpu.roll(value, window - offset, 1)
        value = value[:, :pairs]
        fr, fi = value[0:1], value[1:2]
        vr, vi = vectors_real[:, a : a + 1], vectors_imag[:, a : a + 1]
        moded_real = moded_real + vr * fr - vi * fi
        moded_imag = moded_imag + vi * fr + vr * fi
    high, low = split_wide(jnp.concatenate([moded_real, moded_imag], axis=0))
    both = jnp.concatenate([high, low], axis=0)

    def product(index):
        first = jnp.dot(both, kron[index], preferred_element_type=jnp.float32)
        second = jnp.dot(high, kron[index + 1], preferred_element_type=jnp.float32)
        return first[: 2 * pad] + first[2 * pad :] + second

    by_real = product(0)
    by_imag = product(2)
    out_ref[0, 0] = (by_real[:pad] - by_imag[pad:])[:mode_count]
    out_ref[0, 1] = (by_imag[:pad] + by_real[pad:])[:mode_count]
    for copy in copies:
        copy.wait_send()


def per_device(
    pool,
    rp,
    wannier_coupling,
    lattice_vectors,
    degeneracy,
    fine_points,
    mode_vectors,
    bands_shifted,
    bands_anchor,
):
    rows_here, columns = wannier_coupling.shape[1:]
    points = fine_points.shape[1]
    mode_count = mode_vectors.shape[2]
    pairs = columns // mode_count
    sides = pool // 2
    total = sides * rp
    tiles = -(-columns // LANES)
    height = -(-(2 * tiles + 1) // 8) * 8
    dma = pltpu.SemaphoreType.DMA
    return pl.pallas_call(
        functools.partial(kernel, pool, rp),
        out_shape=jax.ShapeDtypeStruct((1, 2, mode_count, pairs), jnp.float32),
        in_specs=[pl.BlockSpec(memory_space=pl.ANY)] * 7,
        out_specs=pl.BlockSpec(memory_space=pltpu.VMEM),
        scratch_shapes=[
            pltpu.VMEM((2, 2, rows_here, columns), jnp.bfloat16),
            pltpu.VMEM((2, 3, rows_here), jnp.int32),
            pltpu.VMEM((2, 1, rows_here), jnp.int32),
            pltpu.VMEM((sides, 3, points), jnp.int32),
            pltpu.VMEM(mode_vectors.shape[1:], jnp.float32),
            pltpu.VMEM(bands_shifted.shape, jnp.float32),
            pltpu.VMEM(bands_anchor.shape, jnp.float32),
            pltpu.VMEM((total * height, LANES), jnp.float32),
            pltpu.VMEM((total - 1, height, LANES), WIRE),
            pltpu.VMEM((total - 1, height, LANES), WIRE),
            pltpu.VMEM((2, tiles * LANES), jnp.float32),
            pltpu.VMEM((4, pairs, pairs), jnp.bfloat16),
            dma((7,)), dma((3,)), dma((3,)),
            dma((sides - 1,)), dma((sides - 1,)),
            dma((total - 1,)), dma((total - 1,)),
        ],
        compiler_params=pltpu.CompilerParams(
            collective_id=0, has_side_effects=True, vmem_limit_bytes=48 * 1024 * 1024
        ),
    )(wannier_coupling, lattice_vectors, degeneracy, fine_points, mode_vectors, bands_shifted, bands_anchor)


def solution(mesh):
    return jax.shard_map(
        functools.partial(per_device, mesh.shape["pool"], mesh.shape["rp"]),
        mesh=mesh,
        in_specs=(
            P(None, ("pool", "rp"), None),
            P(None, ("pool", "rp")),
            P(None, ("pool", "rp")),
            P(None, "pool"),
            P("pool", None, None, None),
            P(("pool", "rp"), None, None, None),
            P(),
        ),
        out_specs=P(("pool", "rp"), None, None, None),
        check_vma=False,
    )
```

```python
import functools
import math

import jax
import jax.numpy as jnp
from jax import lax
from jax.experimental import pallas as pl
from jax.experimental.pallas import tpu as pltpu
from jax.sharding import PartitionSpec as P

NQG = 48
LANES = 128
SPAN = 1024
WIRE = jnp.int16
TOP = 32000.0

full_turn = 2.0 * math.pi
highest = lax.Precision.HIGHEST
MESH = pl.DeviceIdType.MESH


def split_wide(value):
    high = value.astype(jnp.bfloat16)
    low = (value - high.astype(jnp.float32)).astype(jnp.bfloat16)
    return high, low


def build_pairs(shifted_ref, anchor_ref, kron):
    bands = anchor_ref.shape[1]
    pairs = bands * bands
    row = lax.broadcasted_iota(jnp.int32, (bands, pairs), 0).astype(jnp.float32)
    col = lax.broadcasted_iota(jnp.int32, (bands, pairs), 1).astype(jnp.float32)
    outer = jnp.floor((col + 0.5) * (1.0 / bands))
    inner = col - outer * bands
    pick_outer = jnp.where(row == outer, 1.0, 0.0)
    pick_inner = jnp.where(row == inner, 1.0, 0.0)

    def spread(matrix, pick):
        return jnp.dot(matrix, pick, precision=highest, preferred_element_type=jnp.float32)

    shift_real = spread(shifted_ref[0, 0], pick_outer)
    shift_imag = spread(shifted_ref[0, 1], pick_outer)
    anchor_real = spread(anchor_ref[0], pick_inner)
    anchor_imag = spread(anchor_ref[1], pick_inner)
    for start in range(0, bands, 2):
        reals, imags = [], []
        for m in (start, start + 1):
            sr = shift_real[m : m + 1]
            si = shift_imag[m : m + 1]
            reals.append(sr * anchor_real + si * anchor_imag)
            imags.append(sr * anchor_imag - si * anchor_real)
        rows = pl.ds(start * bands, 2 * bands)
        kron[0, rows, :], kron[1, rows, :] = split_wide(jnp.concatenate(reals, axis=0))
        kron[2, rows, :], kron[3, rows, :] = split_wide(jnp.concatenate(imags, axis=0))


def split_chain(rp):
    low = 1
    while low * low * 4 <= rp:
        low *= 2
    while rp % low:
        low -= 1
    return rp // low, low


def kernel(
    pool,
    rp,
    coupling_ref,
    lattice_ref,
    weight_ref,
    points_ref,
    modes_ref,
    shifted_ref,
    anchor_ref,
    out_ref,
    rows_all,
    lattice,
    weight,
    points,
    modes,
    shifted,
    anchor,
    partial,
    wire,
    recv,
    chain_wire,
    chain_in,
    flat,
    kron,
    load_sem,
    pair_send,
    pair_recv,
    point_send,
    point_recv,
    plane_send,
    plane_recv,
    chain_send,
    chain_recv,
):
    sides = pool // 2
    my_pool = lax.axis_index("pool")
    my_rp = lax.axis_index("rp")
    core = lax.rem(my_pool, 2)
    side = my_pool // 2
    partner = side * 2 + 1 - core
    high_count, low_count = split_chain(rp)
    high, low = my_rp // low_count, lax.rem(my_rp, low_count)
    peers = [(s, shift) for s in range(sides) for shift in range(low_count) if s or shift]
    shifts = sorted(range(high_count), key=lambda shift: -min(shift, high_count - shift))
    pair_id = {"pool": partner, "rp": my_rp}

    def slab_of(other_side, other_high, other_low):
        return (other_side * high_count + other_high) * low_count + other_low

    def plane_peer(step):
        return lax.rem(side + step[0], sides), lax.rem(low + step[1], low_count)

    def device(other_side, other_high, other_low):
        return {"pool": other_side * 2 + core, "rp": other_high * low_count + other_low}

    def chain_peer(shift):
        return lax.rem(high + shift, high_count)

    barrier = pltpu.get_barrier_semaphore()
    for shift in shifts[:-1]:
        pl.semaphore_signal(barrier, inc=1, device_id=device(side, chain_peer(shift), low), device_id_type=MESH)
    for step in peers:
        other_side, other_low = plane_peer(step)
        pl.semaphore_signal(barrier, inc=1, device_id=device(other_side, high, other_low), device_id_type=MESH)
    pl.semaphore_signal(barrier, inc=1, device_id=pair_id, device_id_type=MESH)

    loads = []
    for number, (source, place) in enumerate((
        (coupling_ref, rows_all.at[0]),
        (lattice_ref, lattice.at[0]),
        (weight_ref, weight.at[0]),
        (points_ref, points.at[side]),
        (modes_ref.at[my_rp], modes),
        (shifted_ref, shifted),
        (anchor_ref, anchor),
    )):
        load = pltpu.make_async_copy(source, place, load_sem.at[number])
        load.start()
        loads.append(load)
    loads[5].wait()
    loads[6].wait()
    build_pairs(shifted, anchor, kron)
    for load in loads[:5]:
        load.wait()

    pl.semaphore_wait(barrier, len(peers) + high_count)

    copies = []
    for number, place in enumerate((lattice, weight, rows_all)):
        copy = pltpu.make_async_remote_copy(
            src_ref=place.at[0], dst_ref=place.at[1], send_sem=pair_send.at[number], recv_sem=pair_recv.at[number],
            device_id=pair_id, device_id_type=MESH)
        copy.start()
        copies.append(copy)
    for step in range(1, sides):
        other_side = lax.rem(side + step, sides)
        copy = pltpu.make_async_remote_copy(
            src_ref=points.at[side], dst_ref=points.at[side],
            send_sem=point_send.at[step - 1], recv_sem=point_recv.at[step - 1],
            device_id={"pool": other_side * 2 + core, "rp": my_rp}, device_id_type=MESH)
        copy.start()
        copies.append(copy)
    for copy in copies[:2] + copies[3:]:
        copy.wait()
    here_rows = coupling_ref.shape[1]

    def turn(left, right):
        return lax.dot_general(left, right, (((0,), (0,)), ((), ())), precision=highest, preferred_element_type=jnp.float32)

    def phases(which):
        vectors = lattice[which].astype(jnp.float32)
        winding = jnp.concatenate([turn(points[s].astype(jnp.float32), vectors) for s in range(sides)], axis=0)
        winding = jnp.floor(winding + 0.5)
        winding = winding - NQG * jnp.floor((winding + 0.5) * (1.0 / NQG))
        angles = winding * (full_turn / NQG)
        weights = 1.0 / weight[which].astype(jnp.float32)
        return jnp.cos(angles) * weights, jnp.sin(angles) * weights

    own_real, own_imag = phases(0)
    far_real, far_imag = phases(1)
    left_real = jnp.concatenate([own_real, -own_imag, far_real, -far_imag], axis=1)
    left_imag = jnp.concatenate([own_imag, own_real, far_imag, far_real], axis=1)
    left = jnp.concatenate([left_real, left_imag], axis=0).astype(jnp.bfloat16)
    half = left_real.shape[0]

    copies[2].wait()
    columns = coupling_ref.shape[2]
    height = recv.shape[1]
    largest = jnp.full((half, LANES), 1e-30, jnp.float32)
    for first in range(0, columns, SPAN):
        count = min(SPAN, columns - first)
        block = rows_all[:, :, :, first : first + count].reshape(4 * here_rows, count)
        product = jnp.dot(left, block, preferred_element_type=jnp.float32)
        for begin in range(0, count, LANES):
            size = min(LANES, count - begin)
            piece = product[:, begin : begin + size]
            if size < LANES:
                piece = jnp.concatenate([piece, jnp.zeros((2 * half, LANES - size), jnp.float32)], axis=1)
            row = (first + begin) // LANES * 2
            largest = jnp.maximum(largest, jnp.maximum(jnp.abs(piece[:half]), jnp.abs(piece[half:])))
            for part in range(2):
                partial[pl.ds(row + part, half, stride=height), :] = piece[part * half : (part + 1) * half]

    used = 2 * (-(-columns // LANES))
    largest = jnp.max(jnp.max(largest, axis=0, keepdims=True), axis=1, keepdims=True)
    exponent = jnp.ceil(jnp.log2(largest * (1.0 / TOP)) + 1e-3)
    inverse = jnp.broadcast_to(jnp.exp2(-exponent), (1, LANES))
    exponent = jnp.broadcast_to(exponent, (height, LANES))
    is_value = lax.broadcasted_iota(jnp.int32, (height, LANES), 0) < used

    def slab(index):
        return partial[pl.ds(pl.multiple_of(index * height, 8), height), :]

    def code(values, scale, powers):
        return jnp.round(jnp.where(is_value, values * scale, powers)).astype(jnp.int32).astype(WIRE)

    copies = []
    for shift in shifts:
        other_high = chain_peer(shift)
        for step in peers:
            number = len(copies)
            other_side, other_low = plane_peer(step)
            wire[number] = code(slab(slab_of(other_side, other_high, other_low)), inverse, exponent)
            copies.append(pltpu.make_async_remote_copy(
                src_ref=wire.at[number], dst_ref=recv.at[number],
                send_sem=plane_send.at[number], recv_sem=plane_recv.at[number],
                device_id=device(other_side, high, other_low), device_id_type=MESH))
            if number:
                copies[number - 1].start()
    copies[-1].start()

    room = (len(peers)).bit_length()
    plane_copies = list(copies)
    chain_copies = []
    for place, shift in enumerate(shifts):
        other_high = chain_peer(shift)
        folded = slab(slab_of(side, other_high, low))
        widest = exponent[:1]
        for number in range(place * len(peers), (place + 1) * len(peers)):
            plane_copies[number].wait_recv()
            coded = recv[number].astype(jnp.int32).astype(jnp.float32)
            power = coded[used : used + 1]
            widest = jnp.maximum(widest, power)
            folded = folded + coded * jnp.exp2(power)
        if shift:
            powers = widest + room
            chain_wire[place] = code(folded, jnp.exp2(-powers), jnp.broadcast_to(powers, (height, LANES)))
            copy = pltpu.make_async_remote_copy(
                src_ref=chain_wire.at[place], dst_ref=chain_in.at[place],
                send_sem=chain_send.at[place], recv_sem=chain_recv.at[place],
                device_id=device(side, other_high, low), device_id_type=MESH)
            copy.start()
            chain_copies.append(copy)
    for place, copy in enumerate(chain_copies):
        copy.wait_recv()
        coded = chain_in[place].astype(jnp.int32).astype(jnp.float32)
        folded = folded + coded * jnp.exp2(coded[used : used + 1])
    copies = plane_copies + chain_copies
    for tile in range(flat.shape[1] // LANES):
        flat[:, tile * LANES : (tile + 1) * LANES] = folded[2 * tile : 2 * tile + 2]

    mode_count = modes_ref.shape[1]
    pad = -(-mode_count // 8) * 8
    pairs = out_ref.shape[3]
    window = -(-(pairs + LANES // 2) // LANES) * LANES
    unit_row = lax.broadcasted_iota(jnp.int32, (mode_count, LANES), 0)
    unit_col = lax.broadcasted_iota(jnp.int32, (mode_count, LANES), 1)
    unit = jnp.where(unit_row == unit_col, 1.0, 0.0)
    empty = jnp.zeros((pad - mode_count, LANES), jnp.float32)
    vectors_real = jnp.concatenate([turn(modes[:, 0, :], unit), empty], axis=0)
    vectors_imag = jnp.concatenate([turn(modes[:, 1, :], unit), empty], axis=0)
    moded_real = jnp.zeros((vectors_real.shape[0], pairs), jnp.float32)
    moded_imag = moded_real
    for a in range(mode_count):
        offset = a * pairs % LANES
        begin = a * pairs - offset
        value = flat[:, begin : begin + window]
        if offset:
            value = pltpu.roll(value, window - offset, 1)
        value = value[:, :pairs]
        fr, fi = value[0:1], value[1:2]
        vr, vi = vectors_real[:, a : a + 1], vectors_imag[:, a : a + 1]
        moded_real = moded_real + vr * fr - vi * fi
        moded_imag = moded_imag + vi * fr + vr * fi
    coarse, rest = split_wide(jnp.concatenate([moded_real, moded_imag], axis=0))
    both = jnp.concatenate([coarse, rest], axis=0)

    def product(index):
        first = jnp.dot(both, kron[index], preferred_element_type=jnp.float32)
        second = jnp.dot(coarse, kron[index + 1], preferred_element_type=jnp.float32)
        return first[: 2 * pad] + first[2 * pad :] + second

    by_real = product(0)
    by_imag = product(2)
    out_ref[0, :, 0, :] = (by_real[:pad] - by_imag[pad:])[:mode_count]
    out_ref[0, :, 1, :] = (by_imag[:pad] + by_real[pad:])[:mode_count]
    for copy in copies:
        copy.wait_send()


def per_device(
    pool,
    rp,
    wannier_coupling,
    lattice_vectors,
    degeneracy,
    fine_points,
    mode_vectors,
    bands_shifted,
    bands_anchor,
):
    rows_here, columns = wannier_coupling.shape[1:]
    points = fine_points.shape[1]
    mode_count = mode_vectors.shape[2]
    pairs = columns // mode_count
    sides = pool // 2
    total = sides * rp
    tiles = -(-columns // LANES)
    height = -(-(2 * tiles + 1) // 8) * 8
    dma = pltpu.SemaphoreType.DMA
    high_count, low_count = split_chain(rp)
    plane = high_count * (sides * low_count - 1)
    result = pl.pallas_call(
        functools.partial(kernel, pool, rp),
        out_shape=jax.ShapeDtypeStruct((1, mode_count, 2, pairs), jnp.float32),
        in_specs=[pl.BlockSpec(memory_space=pl.ANY)] * 7,
        out_specs=pl.BlockSpec(memory_space=pltpu.VMEM),
        scratch_shapes=[
            pltpu.VMEM((2, 2, rows_here, columns), jnp.bfloat16),
            pltpu.VMEM((2, 3, rows_here), jnp.int32),
            pltpu.VMEM((2, 1, rows_here), jnp.int32),
            pltpu.VMEM((sides, 3, points), jnp.int32),
            pltpu.VMEM((mode_count, 2, mode_count), jnp.float32),
            pltpu.VMEM(bands_shifted.shape, jnp.float32),
            pltpu.VMEM(bands_anchor.shape, jnp.float32),
            pltpu.VMEM((total * height, LANES), jnp.float32),
            pltpu.VMEM((plane, height, LANES), WIRE),
            pltpu.VMEM((plane, height, LANES), WIRE),
            pltpu.VMEM((high_count - 1, height, LANES), WIRE),
            pltpu.VMEM((high_count - 1, height, LANES), WIRE),
            pltpu.VMEM((2, tiles * LANES), jnp.float32),
            pltpu.VMEM((4, pairs, pairs), jnp.bfloat16),
            dma((7,)), dma((3,)), dma((3,)),
            dma((sides - 1,)), dma((sides - 1,)),
            dma((plane,)), dma((plane,)),
            dma((high_count - 1,)), dma((high_count - 1,)),
        ],
        compiler_params=pltpu.CompilerParams(
            collective_id=0, has_side_effects=True, vmem_limit_bytes=67043328
        ),
    )(wannier_coupling, lattice_vectors, degeneracy, fine_points, jnp.swapaxes(mode_vectors, 1, 2), bands_shifted, bands_anchor)
    return jnp.swapaxes(result, 1, 2)


def solution(mesh):
    return jax.shard_map(
        functools.partial(per_device, mesh.shape["pool"], mesh.shape["rp"]),
        mesh=mesh,
        in_specs=(
            P(None, ("pool", "rp"), None),
            P(None, ("pool", "rp")),
            P(None, ("pool", "rp")),
            P(None, "pool"),
            P("pool", None, None, None),
            P(("pool", "rp"), None, None, None),
            P(),
        ),
        out_specs=P(("pool", "rp"), None, None, None),
        check_vma=False,
    )
```

```python
import functools
import math

import jax
import jax.numpy as jnp
from jax import lax
from jax.experimental import pallas as pl
from jax.experimental.pallas import tpu as pltpu
from jax.sharding import PartitionSpec as P

NQG = 48
LANES = 128
SPAN = 1024
WIRE = jnp.int16
TOP = 32000.0

full_turn = 2.0 * math.pi
highest = lax.Precision.HIGHEST
MESH = pl.DeviceIdType.MESH


def split_wide(value):
    high = value.astype(jnp.bfloat16)
    low = (value - high.astype(jnp.float32)).astype(jnp.bfloat16)
    return high, low


def build_pairs(shifted_ref, anchor_ref, kron):
    bands = anchor_ref.shape[1]
    pairs = bands * bands
    row = lax.broadcasted_iota(jnp.int32, (bands, pairs), 0).astype(jnp.float32)
    col = lax.broadcasted_iota(jnp.int32, (bands, pairs), 1).astype(jnp.float32)
    outer = jnp.floor((col + 0.5) * (1.0 / bands))
    inner = col - outer * bands
    pick_outer = jnp.where(row == outer, 1.0, 0.0)
    pick_inner = jnp.where(row == inner, 1.0, 0.0)

    def spread(matrix, pick):
        return jnp.dot(matrix, pick, precision=highest, preferred_element_type=jnp.float32)

    shift_real = spread(shifted_ref[0, 0], pick_outer)
    shift_imag = spread(shifted_ref[0, 1], pick_outer)
    anchor_real = spread(anchor_ref[0], pick_inner)
    anchor_imag = spread(anchor_ref[1], pick_inner)
    for start in range(0, bands, 2):
        reals, imags = [], []
        for m in (start, start + 1):
            sr = shift_real[m : m + 1]
            si = shift_imag[m : m + 1]
            reals.append(sr * anchor_real + si * anchor_imag)
            imags.append(sr * anchor_imag - si * anchor_real)
        rows = pl.ds(start * bands, 2 * bands)
        kron[0, rows, :], kron[1, rows, :] = split_wide(jnp.concatenate(reals, axis=0))
        kron[2, rows, :], kron[3, rows, :] = split_wide(jnp.concatenate(imags, axis=0))


def split_chain(rp):
    low = 1
    while low * low * 4 <= rp:
        low *= 2
    while rp % low:
        low -= 1
    return rp // low, low


def kernel(
    pool,
    rp,
    coupling_ref,
    lattice_ref,
    weight_ref,
    points_ref,
    modes_ref,
    shifted_ref,
    anchor_ref,
    out_ref,
    rows_all,
    lattice,
    weight,
    points,
    modes,
    shifted,
    anchor,
    partial,
    wire,
    recv,
    chain_wire,
    chain_in,
    flat,
    kron,
    load_sem,
    pair_send,
    pair_recv,
    point_send,
    point_recv,
    plane_send,
    plane_recv,
    chain_send,
    chain_recv,
):
    sides = pool // 2
    my_pool = lax.axis_index("pool")
    my_rp = lax.axis_index("rp")
    core = lax.rem(my_pool, 2)
    side = my_pool // 2
    partner = side * 2 + 1 - core
    high_count, low_count = split_chain(rp)
    high, low = my_rp // low_count, lax.rem(my_rp, low_count)
    peers = [(s, shift) for s in range(sides) for shift in range(low_count) if s or shift]
    shifts = sorted(range(high_count), key=lambda shift: -min(shift, high_count - shift))
    pair_id = {"pool": partner, "rp": my_rp}

    def slab_of(other_side, other_high, other_low):
        return (other_side * high_count + other_high) * low_count + other_low

    def plane_peer(step):
        return lax.rem(side + step[0], sides), lax.rem(low + step[1], low_count)

    def device(other_side, other_high, other_low):
        return {"pool": other_side * 2 + core, "rp": other_high * low_count + other_low}

    def chain_peer(shift):
        return lax.rem(high + shift, high_count)

    barrier = pltpu.get_barrier_semaphore()
    for shift in shifts[:-1]:
        pl.semaphore_signal(barrier, inc=1, device_id=device(side, chain_peer(shift), low), device_id_type=MESH)
    for step in peers:
        other_side, other_low = plane_peer(step)
        pl.semaphore_signal(barrier, inc=1, device_id=device(other_side, high, other_low), device_id_type=MESH)
    pl.semaphore_signal(barrier, inc=1, device_id=pair_id, device_id_type=MESH)

    loads = []
    for number, (source, place) in enumerate((
        (coupling_ref, rows_all.at[0]),
        (lattice_ref, lattice.at[0]),
        (weight_ref, weight.at[0]),
        (points_ref, points.at[side]),
        (modes_ref.at[my_rp], modes),
        (shifted_ref, shifted),
        (anchor_ref, anchor),
    )):
        load = pltpu.make_async_copy(source, place, load_sem.at[number])
        load.start()
        loads.append(load)
    loads[5].wait()
    loads[6].wait()
    build_pairs(shifted, anchor, kron)
    for load in loads[:5]:
        load.wait()

    pl.semaphore_wait(barrier, len(peers) + high_count)

    copies = []
    for step in range(1, sides):
        other_side = lax.rem(side + step, sides)
        copy = pltpu.make_async_remote_copy(
            src_ref=points.at[side], dst_ref=points.at[side],
            send_sem=point_send.at[step - 1], recv_sem=point_recv.at[step - 1],
            device_id={"pool": other_side * 2 + core, "rp": my_rp}, device_id_type=MESH)
        copy.start()
        copies.append(copy)
    for number, place in enumerate((lattice, weight, rows_all)):
        copy = pltpu.make_async_remote_copy(
            src_ref=place.at[0], dst_ref=place.at[1], send_sem=pair_send.at[number], recv_sem=pair_recv.at[number],
            device_id=pair_id, device_id_type=MESH)
        copy.start()
        copies.append(copy)
    for copy in copies[:-1]:
        copy.wait()
    here_rows = coupling_ref.shape[1]

    def turn(left, right):
        return lax.dot_general(left, right, (((0,), (0,)), ((), ())), precision=highest, preferred_element_type=jnp.float32)

    def phases(which):
        vectors = lattice[which].astype(jnp.float32)
        winding = jnp.concatenate([turn(points[s].astype(jnp.float32), vectors) for s in range(sides)], axis=0)
        winding = jnp.floor(winding + 0.5)
        winding = winding - NQG * jnp.floor((winding + 0.5) * (1.0 / NQG))
        angles = winding * (full_turn / NQG)
        weights = 1.0 / weight[which].astype(jnp.float32)
        return jnp.cos(angles) * weights, jnp.sin(angles) * weights

    own_real, own_imag = phases(0)
    far_real, far_imag = phases(1)
    left_real = jnp.concatenate([own_real, -own_imag, far_real, -far_imag], axis=1)
    left_imag = jnp.concatenate([own_imag, own_real, far_imag, far_real], axis=1)
    left = jnp.concatenate([left_real, left_imag], axis=0).astype(jnp.bfloat16)
    half = left_real.shape[0]

    copies[-1].wait()
    columns = coupling_ref.shape[2]
    height = recv.shape[1]
    largest = jnp.full((half, LANES), 1e-30, jnp.float32)
    for first in range(0, columns, SPAN):
        count = min(SPAN, columns - first)
        block = rows_all[:, :, :, first : first + count].reshape(4 * here_rows, count)
        product = jnp.dot(left, block, preferred_element_type=jnp.float32)
        for begin in range(0, count, LANES):
            size = min(LANES, count - begin)
            piece = product[:, begin : begin + size]
            if size < LANES:
                piece = jnp.concatenate([piece, jnp.zeros((2 * half, LANES - size), jnp.float32)], axis=1)
            row = (first + begin) // LANES * 2
            largest = jnp.maximum(largest, jnp.maximum(jnp.abs(piece[:half]), jnp.abs(piece[half:])))
            for part in range(2):
                partial[pl.ds(row + part, half, stride=height), :] = piece[part * half : (part + 1) * half]

    used = 2 * (-(-columns // LANES))
    largest = jnp.max(jnp.max(largest, axis=0, keepdims=True), axis=1, keepdims=True)
    exponent = jnp.ceil(jnp.log2(largest * (1.0 / TOP)) + 1e-3)
    inverse = jnp.broadcast_to(jnp.exp2(-exponent), (1, LANES))
    exponent = jnp.broadcast_to(exponent, (height, LANES))
    is_value = lax.broadcasted_iota(jnp.int32, (height, LANES), 0) < used

    def slab(index):
        return partial[pl.ds(pl.multiple_of(index * height, 8), height), :]

    def code(values, scale, powers):
        return jnp.round(jnp.where(is_value, values * scale, powers)).astype(jnp.int32).astype(WIRE)

    copies = []
    for shift in shifts:
        other_high = chain_peer(shift)
        for step in peers:
            number = len(copies)
            other_side, other_low = plane_peer(step)
            wire[number] = code(slab(slab_of(other_side, other_high, other_low)), inverse, exponent)
            copies.append(pltpu.make_async_remote_copy(
                src_ref=wire.at[number], dst_ref=recv.at[number],
                send_sem=plane_send.at[number], recv_sem=plane_recv.at[number],
                device_id=device(other_side, high, other_low), device_id_type=MESH))
            if number:
                copies[number - 1].start()
    copies[-1].start()

    room = (len(peers)).bit_length()
    plane_copies = list(copies)
    chain_copies = []
    for place, shift in enumerate(shifts):
        other_high = chain_peer(shift)
        folded = slab(slab_of(side, other_high, low))
        widest = exponent[:1]
        for number in range(place * len(peers), (place + 1) * len(peers)):
            plane_copies[number].wait_recv()
            coded = recv[number].astype(jnp.int32).astype(jnp.float32)
            power = coded[used : used + 1]
            widest = jnp.maximum(widest, power)
            folded = folded + coded * jnp.exp2(power)
        if shift:
            powers = widest + room
            chain_wire[place] = code(folded, jnp.exp2(-powers), jnp.broadcast_to(powers, (height, LANES)))
            copy = pltpu.make_async_remote_copy(
                src_ref=chain_wire.at[place], dst_ref=chain_in.at[place],
                send_sem=chain_send.at[place], recv_sem=chain_recv.at[place],
                device_id=device(side, other_high, low), device_id_type=MESH)
            copy.start()
            chain_copies.append(copy)
    for place, copy in enumerate(chain_copies):
        copy.wait_recv()
        coded = chain_in[place].astype(jnp.int32).astype(jnp.float32)
        folded = folded + coded * jnp.exp2(coded[used : used + 1])
    copies = plane_copies + chain_copies
    for tile in range(flat.shape[1] // LANES):
        flat[:, tile * LANES : (tile + 1) * LANES] = folded[2 * tile : 2 * tile + 2]

    mode_count = modes_ref.shape[1]
    pad = -(-mode_count // 8) * 8
    pairs = out_ref.shape[3]
    window = -(-(pairs + LANES // 2) // LANES) * LANES
    unit_row = lax.broadcasted_iota(jnp.int32, (mode_count, LANES), 0)
    unit_col = lax.broadcasted_iota(jnp.int32, (mode_count, LANES), 1)
    unit = jnp.where(unit_row == unit_col, 1.0, 0.0)
    empty = jnp.zeros((pad - mode_count, LANES), jnp.float32)
    vectors_real = jnp.concatenate([turn(modes[:, 0, :], unit), empty], axis=0)
    vectors_imag = jnp.concatenate([turn(modes[:, 1, :], unit), empty], axis=0)
    moded_real = jnp.zeros((vectors_real.shape[0], pairs), jnp.float32)
    moded_imag = moded_real
    for a in range(mode_count):
        offset = a * pairs % LANES
        begin = a * pairs - offset
        value = flat[:, begin : begin + window]
        if offset:
            value = pltpu.roll(value, window - offset, 1)
        value = value[:, :pairs]
        fr, fi = value[0:1], value[1:2]
        vr, vi = vectors_real[:, a : a + 1], vectors_imag[:, a : a + 1]
        moded_real = moded_real + vr * fr - vi * fi
        moded_imag = moded_imag + vi * fr + vr * fi
    coarse, rest = split_wide(jnp.concatenate([moded_real, moded_imag], axis=0))
    both = jnp.concatenate([coarse, rest], axis=0)

    def product(index):
        first = jnp.dot(both, kron[index], preferred_element_type=jnp.float32)
        second = jnp.dot(coarse, kron[index + 1], preferred_element_type=jnp.float32)
        return first[: 2 * pad] + first[2 * pad :] + second

    by_real = product(0)
    by_imag = product(2)
    out_ref[0, :, 0, :] = (by_real[:pad] - by_imag[pad:])[:mode_count]
    out_ref[0, :, 1, :] = (by_imag[:pad] + by_real[pad:])[:mode_count]
    for copy in copies:
        copy.wait_send()


def per_device(
    pool,
    rp,
    wannier_coupling,
    lattice_vectors,
    degeneracy,
    fine_points,
    mode_vectors,
    bands_shifted,
    bands_anchor,
):
    rows_here, columns = wannier_coupling.shape[1:]
    points = fine_points.shape[1]
    mode_count = mode_vectors.shape[2]
    pairs = columns // mode_count
    sides = pool // 2
    total = sides * rp
    tiles = -(-columns // LANES)
    height = -(-(2 * tiles + 1) // 8) * 8
    dma = pltpu.SemaphoreType.DMA
    high_count, low_count = split_chain(rp)
    plane = high_count * (sides * low_count - 1)
    result = pl.pallas_call(
        functools.partial(kernel, pool, rp),
        out_shape=jax.ShapeDtypeStruct((1, mode_count, 2, pairs), jnp.float32),
        in_specs=[pl.BlockSpec(memory_space=pl.ANY)] * 7,
        out_specs=pl.BlockSpec(memory_space=pltpu.VMEM),
        scratch_shapes=[
            pltpu.VMEM((2, 2, rows_here, columns), jnp.bfloat16),
            pltpu.VMEM((2, 3, rows_here), jnp.int32),
            pltpu.VMEM((2, 1, rows_here), jnp.int32),
            pltpu.VMEM((sides, 3, points), jnp.int32),
            pltpu.VMEM((mode_count, 2, mode_count), jnp.float32),
            pltpu.VMEM(bands_shifted.shape, jnp.float32),
            pltpu.VMEM(bands_anchor.shape, jnp.float32),
            pltpu.VMEM((total * height, LANES), jnp.float32),
            pltpu.VMEM((plane, height, LANES), WIRE),
            pltpu.VMEM((plane, height, LANES), WIRE),
            pltpu.VMEM((high_count - 1, height, LANES), WIRE),
            pltpu.VMEM((high_count - 1, height, LANES), WIRE),
            pltpu.VMEM((2, tiles * LANES), jnp.float32),
            pltpu.VMEM((4, pairs, pairs), jnp.bfloat16),
            dma((7,)), dma((3,)), dma((3,)),
            dma((sides - 1,)), dma((sides - 1,)),
            dma((plane,)), dma((plane,)),
            dma((high_count - 1,)), dma((high_count - 1,)),
        ],
        compiler_params=pltpu.CompilerParams(
            collective_id=0, has_side_effects=True, vmem_limit_bytes=67043328
        ),
    )(wannier_coupling, lattice_vectors, degeneracy, fine_points, jnp.swapaxes(mode_vectors, 1, 2), bands_shifted, bands_anchor)
    return jnp.swapaxes(result, 1, 2)


def solution(mesh):
    return jax.shard_map(
        functools.partial(per_device, mesh.shape["pool"], mesh.shape["rp"]),
        mesh=mesh,
        in_specs=(
            P(None, ("pool", "rp"), None),
            P(None, ("pool", "rp")),
            P(None, ("pool", "rp")),
            P(None, "pool"),
            P("pool", None, None, None),
            P(("pool", "rp"), None, None, None),
            P(),
        ),
        out_specs=P(("pool", "rp"), None, None, None),
        check_vma=False,
    )
```
